512 devices in a mesh: gx: 8 (over y_lo, core), gy: 8 (over z), gz: 8 (over y_hi, x).
Axes of the slice: x: 4, y: 8 (y_hi: 2, y_lo: 4; y = y_hi * 4 + y_lo), z: 8, core: 2. Of those that a mesh axis runs over, the one named last changes fastest.
Arguments:
- right_side: bfloat16 [262144, 1024], P(('gx', 'gy', 'gz')), may hold values from -6 to 6
- projector: bfloat16 [262144, 256], P(('gx', 'gy', 'gz')), may hold values from -0.25 to 0.25
- translations: bfloat16 [512, 9, 256, 512], P(('gx', 'gy', 'gz')), may hold values from -0.25 to 0.25
- evaluator: bfloat16 [262144, 256], P(('gx', 'gy', 'gz')), may hold values from -0.375 to 0.375
Outputs:
- product: bfloat16 [262144, 1024], P(('gx', 'gy', 'gz'))
The draws below stay inside these ranges and needn't reach their ends.
All inputs are finite; a program needn't handle non-finite values.
Results may differ from the reference program's by a relative error of at most 0.02.
Values may be sent and summed in bfloat16 or wider, within the bound.
No kernel may reach another device: no remote copies, remote signals or barrier semaphores. Data moves between devices by JAX's collectives and lax.ppermute only.
A program may use at most 64 MiB of HBM per device.

```python
import jax
import jax.numpy as jnp
from jax import lax

RANK = 256
RHS = 1024
LEAF = 512
BOXES = 512
ROWS = 262144
BITS_GX = 3
BITS_GY = 3
BITS_GZ = 3
LEVELS = 9
N_GY = 8
N_GZ = 8


def block_levels(key, extent, split, least, high):
    loudness = 1.0
    for position, shards_of in split:
        steps = jax.random.uniform(jax.random.fold_in(jax.random.fold_in(key, 6), position), (shards_of,), jnp.float32, least / len(split), high / len(split))
        loudness = loudness * jnp.repeat(jnp.exp(steps), extent[position] // shards_of).reshape((-1,) + (1,) * (len(extent) - 1 - position))
    return loudness


def normal_values(own_key, dims, width, bound, split=(), dtype=jnp.bfloat16):
    factor_of = block_levels(own_key, dims, split, -0.22, 0.18) if split else 1.0
    values = jax.random.normal(own_key, dims, jnp.float32) * width * factor_of
    return jnp.minimum(jnp.maximum(values, -bound), bound).astype(dtype)


def setup_inputs(seed: int = 0) -> dict:
    arg_keys = jax.random.split(jax.random.key(seed), 5)
    right_side = normal_values(arg_keys[0], (ROWS, RHS), 1.0, 6.0, ((0, 512),))
    projector = normal_values(arg_keys[1], (ROWS, RANK), LEAF ** -0.5, 0.25, ((0, 512),))
    translations = normal_values(arg_keys[2], (BOXES, LEVELS, RANK, 2 * RANK), (2 * RANK) ** -0.5, 0.25, ((0, 512),))
    evaluator = normal_values(arg_keys[3], (ROWS, RANK), RANK ** -0.5, 0.375, ((0, 512),))
    return {"right_side": right_side, "projector": projector, "translations": translations, "evaluator": evaluator}


def project_box(bundle):
    return jnp.dot(bundle[0].T, bundle[1], preferred_element_type=jnp.float32).astype(jnp.bfloat16)


def translate_box(bundle):
    mapping, own_part, partner = bundle
    total = jnp.dot(mapping[:, :RANK], own_part, preferred_element_type=jnp.float32)
    total = total + jnp.dot(mapping[:, RANK:], partner, preferred_element_type=jnp.float32)
    return total.astype(jnp.bfloat16)


def evaluate_box(bundle):
    return jnp.dot(bundle[0], bundle[1], preferred_element_type=jnp.float32).astype(jnp.bfloat16)


def reference(right_side, projector, translations, evaluator):
    source_rows = right_side.reshape(BOXES, LEAF, RHS)
    project_rows = projector.reshape(BOXES, LEAF, RANK)
    evaluate_rows = evaluator.reshape(BOXES, LEAF, RANK)
    coefficients = lax.map(project_box, (project_rows, source_rows))
    strides = [N_GY * N_GZ * 2 ** k for k in range(BITS_GX)]
    strides = strides + [N_GZ * 2 ** k for k in range(BITS_GY)]
    strides = strides + [2 ** k for k in range(BITS_GZ)]
    for height, stride in enumerate(strides):
        viewed = coefficients.reshape(BOXES // (2 * stride), 2, stride, RANK, RHS)
        partner = viewed[:, ::-1].reshape(BOXES, RANK, RHS)
        coefficients = lax.map(translate_box, (translations[:, height], coefficients, partner))
    result = lax.map(evaluate_box, (evaluate_rows, coefficients))
    return result.reshape(ROWS, RHS)
```

```python
import jax
import jax.numpy as jnp
from jax import lax
from jax.experimental import pallas as pl
from jax.experimental.pallas import tpu as pltpu
from jax.sharding import PartitionSpec as P

BLOCKS = 2
NEAR = True
NANOS = 14000


def swap(block, axis, stride):
    count = lax.axis_size(axis)
    return lax.ppermute(block, axis, [(i, i ^ stride) for i in range(count)])


def times(rows, matrix):
    return lax.dot_general(rows, matrix, (((1,), (1,)), ((), ())), preferred_element_type=jnp.float32)


def mix(first, second, mapping):
    rank = mapping.shape[0]
    return (times(first, mapping[:, :rank]) + times(second, mapping[:, rank:])).astype(jnp.bfloat16)


def hold_second_core(blocks):
    def wait(*refs):
        @pl.when(lax.axis_index("gx") % 2 == 1)
        def _():
            pl.delay(NANOS)

    anywhere = [pl.BlockSpec(memory_space=pl.ANY)] * len(blocks)
    return list(pl.pallas_call(
        wait,
        out_shape=[jax.ShapeDtypeStruct(rows.shape, rows.dtype) for rows in blocks],
        in_specs=anywhere,
        out_specs=anywhere,
        input_output_aliases={k: k for k in range(len(blocks))},
    )(*blocks))


def body(right_side, projector, translations, evaluator):
    maps = translations[0]
    size = right_side.shape[1] // BLOCKS
    blocks = [
        lax.dot_general(
            right_side[:, k * size : (k + 1) * size], projector, (((0,), (0,)), ((), ())),
            preferred_element_type=jnp.float32,
        ).astype(jnp.bfloat16)
        for k in range(BLOCKS)
    ]
    if NEAR:
        map_4_near = swap(maps[4], "gy", 2)
    level = 0
    for axis in ("gx", "gy", "gz"):
        for bit in range(3):
            sent, stride = blocks, 1 << bit
            if NEAR and level == 5:
                sent, stride = beside, 6
            others = [swap(rows, axis, stride) for rows in sent]
            if NEAR and level == 4:
                beside = [mix(other, rows, map_4_near) for rows, other in zip(blocks, others)]
            blocks = [mix(rows, other, maps[level]) for rows, other in zip(blocks, others)]
            if level == 0 and NANOS:
                blocks = hold_second_core(blocks)
            level += 1
    outs = [lax.dot_general(
        evaluator, rows, (((1,), (1,)), ((), ())), preferred_element_type=jnp.float32
    ).astype(jnp.bfloat16) for rows in blocks]
    return jnp.concatenate(outs, axis=1)


def solution(mesh):
    placed = (
        P(("gx", "gy", "gz"), None),
        P(("gx", "gy", "gz"), None),
        P(("gx", "gy", "gz"), None, None, None),
        P(("gx", "gy", "gz"), None),
    )
    return jax.shard_map(
        body, mesh=mesh, in_specs=placed, out_specs=P(("gx", "gy", "gz"), None), check_vma=False
    )
```

```python
import jax
import jax.numpy as jnp
from jax import lax
from jax.experimental import pallas as pl
from jax.experimental.pallas import tpu as pltpu
from jax.sharding import PartitionSpec as P

BLOCKS = 2
LATE = 3
HELD = 2
TOGETHER = False
NEAR = True
NANOS = 14500


def swap(block, axis, stride):
    count = lax.axis_size(axis)
    return lax.ppermute(block, axis, [(i, i ^ stride) for i in range(count)])


def times(rows, matrix):
    return lax.dot_general(rows, matrix, (((1,), (1,)), ((), ())), preferred_element_type=jnp.float32)


def mix(first, second, mapping):
    rank = mapping.shape[0]
    return (times(first, mapping[:, :rank]) + times(second, mapping[:, rank:])).astype(jnp.bfloat16)


def hold_second_core(blocks):
    def wait(*refs):
        @pl.when(lax.axis_index("gx") % 2 == 1)
        def _():
            pl.delay(NANOS)

    anywhere = [pl.BlockSpec(memory_space=pl.ANY)] * len(blocks)
    return list(pl.pallas_call(
        wait,
        out_shape=[jax.ShapeDtypeStruct(rows.shape, rows.dtype) for rows in blocks],
        in_specs=anywhere,
        out_specs=anywhere,
        input_output_aliases={k: k for k in range(len(blocks))},
    )(*blocks))


def body(right_side, projector, translations, evaluator):
    maps = translations[0]
    size = right_side.shape[1] // BLOCKS
    blocks = [
        lax.dot_general(
            right_side[:, k * size : (k + 1) * size], projector, (((0,), (0,)), ((), ())),
            preferred_element_type=jnp.float32,
        ).astype(jnp.bfloat16)
        for k in range(BLOCKS)
    ]
    if NEAR:
        map_4_near = swap(maps[4], "gy", 2)
    maps = [maps[k] for k in range(maps.shape[0])]
    level = 0
    for axis in ("gx", "gy", "gz"):
        for bit in range(3):
            sent, stride = blocks, 1 << bit
            if NEAR and level == 5:
                sent, stride = beside, 6
            others = [swap(rows, axis, stride) for rows in sent]
            if NEAR and level == 4:
                pairs = zip(blocks, others)
                if TOGETHER:
                    pairs = [lax.optimization_barrier(pair) for pair in pairs]
                beside = [mix(other, rows, map_4_near) for rows, other in pairs]
            blocks = [mix(rows, other, maps[level]) for rows, other in zip(blocks, others)]
            if level == 0 and NANOS:
                blocks = [*hold_second_core(blocks[:HELD]), *blocks[HELD:]]
            if level == LATE:
                late, blocks[0] = lax.optimization_barrier((translations, blocks[0]))
                maps[6:] = [late[0, k] for k in range(6, 9)]
            level += 1
    outs = [lax.dot_general(
        evaluator, rows, (((1,), (1,)), ((), ())), preferred_element_type=jnp.float32
    ).astype(jnp.bfloat16) for rows in blocks]
    return jnp.concatenate(outs, axis=1)


def solution(mesh):
    placed = (
        P(("gx", "gy", "gz"), None),
        P(("gx", "gy", "gz"), None),
        P(("gx", "gy", "gz"), None, None, None),
        P(("gx", "gy", "gz"), None),
    )
    return jax.shard_map(
        body, mesh=mesh, in_specs=placed, out_specs=P(("gx", "gy", "gz"), None), check_vma=False
    )
```
